32 devices in a mesh: groups: 2 (over y), seq: 4 (over z), section: 2 (over x), tp: 2 (over core).
Axes of the slice: x: 2, y: 2, z: 4, core: 2. Of those that a mesh axis runs over, the one named last changes fastest.
Arguments:
- qkv: bfloat16 [4, 1024, 3, 2048], P(('groups', 'section'), ('seq', 'tp')), parts along dimension 0, may hold values from -100 to 100
- stream: bfloat16 [4, 1024, 3072], P(('groups', 'section'), ('seq', 'tp')), parts along dimension 0, may hold values from -6 to 6
- out_weight: bfloat16 [2048, 3072], P('tp'), may hold values from -0.125 to 0.125
- mod_scale: float32 [4, 3072], P(('groups', 'section')), parts along dimension 0, may hold values from -3 to 3
- mod_shift: float32 [4, 3072], P(('groups', 'section')), parts along dimension 0, may hold values from -3 to 3
- final_weight: bfloat16 [3072, 64], replicated, may hold values from -0.109375 to 0.109375
- latent: float32 [4, 1024, 64], P(('groups', 'section'), ('seq', 'tp')), parts along dimension 0, may hold values from -6 to 6
- step_size: float32 [4], P(('groups', 'section')), parts along dimension 0, may hold values from 0.2 to 1
- frame_counts: int32 [4, 4], P(('groups', 'section')), parts along dimension 0, may hold values from 1 to 4, 8 in all within a row
- finished: int32 [4, 4], P(('groups', 'section')), parts along dimension 0, may hold values 0 or 1
- conv_weight: bfloat16 [3, 3, 3, 16, 512], P(None, None, None, None, 'tp'), may hold values from -0.3125 to 0.3125
- conv_bias: float32 [512], P('tp'), may hold values from -3 to 3
- up_weight: bfloat16 [512, 512], P('tp'), may hold values from -0.25 to 0.25
- up_bias: float32 [512], P('tp'), may hold values from -3 to 3
Outputs:
- new_latent: float32 [4, 1024, 64], P(('groups', 'section'), ('seq', 'tp')), parts along dimension 0
- decoded: bfloat16 [4, 8, 16, 32, 512], P(('groups', 'section'), None, 'seq', None, 'tp'), parts along dimension 0
The draws below stay inside these ranges and needn't reach their ends.
There are 2 independent parts, one for each index of `groups`. The reference program is written for one: setup_inputs(seed, part) draws one part's arguments, and reference() takes and returns one part's arrays. A program takes and returns all parts, laid end to end along the dimension named above; an argument that names none is the same for every part. Nothing has to cross between parts.
Inputs may be any that keep to these rules, and one draw needn't show every extreme that they name: `frame_counts`: a part's 4 requests are packed in order and their frame counts sum to 8.
All inputs are finite; a program needn't handle non-finite values. No bound on the sum of `finished` on one device may be relied on, other than what follows from the above.
Results may differ from the reference program's by a relative error of at most 0.012.
Values may be sent and summed in bfloat16 or wider, within the bound.
A program may use at most 64 MiB of HBM per device.

```python
import math
import jax
import jax.numpy as jnp
import numpy as np
from jax import lax

D = 3072
HEADS = 16
HD = 128
LATC = 16
PATCH = 64
VAEC = 512
UPC = 512
PROWS = 8
PCOLS = 16
REQ = 4
F_TOK = 128
LROWS = 16
LCOLS = 32
FRAMES = 8
TOKS = 1024
MAXF = 4
N_SECTION = 2


def draw_qkv(key, part):
    array_dims = (N_SECTION, TOKS, 3, HEADS * HD)
    base = jnp.clip(jax.random.normal(key, array_dims, jnp.float32), -4.0, 4.0)
    return base.astype(jnp.bfloat16)


def with_ends(entries, key, smallest, high):
    index_at = [jax.random.randint(jax.random.fold_in(key, axis), (), 0, length) for axis, length in enumerate(entries.shape)]
    longest = entries.shape.index(max(entries.shape))
    neighbour = index_at[:longest] + [(index_at[longest] + 1) % entries.shape[longest]] + index_at[longest + 1:]
    return entries.at[tuple(index_at)].set(smallest).at[tuple(neighbour)].set(high)


def level_of(rng, shape, split, least, high):
    gain, own = 1.0, jax.random.fold_in(rng, 6)
    for position, parts in split:
        heights = jnp.exp(jax.random.uniform(jax.random.fold_in(own, position), (parts,), jnp.float32, least / len(split), high / len(split)))
        gain = gain * jnp.repeat(heights, shape[position] // parts).reshape([-1 if axis == position else 1 for axis in range(len(shape))])
    return gain


def profile(amount, total, bound, lean):
    weights = [(1 << 20) // math.isqrt(rank ** lean) + 1 for rank in range(2, amount + 1)]
    surplus, given = total - bound - (amount - 1), [1] * (amount - 1)
    while surplus > 0:
        free = [i for i in range(amount - 1) if given[i] < bound]
        whole, budget = sum([weights[i] for i in free]), surplus
        for i in free:
            extra = min(bound - given[i], max(1, budget * weights[i] // whole), surplus)
            given[i] = given[i] + extra
            surplus = surplus - extra
    return np.array([bound] + given)


def uneven_parts(key, number_of, total, reach, lean):
    if number_of == 2:
        one = jax.random.randint(key, (), max(1, total - reach), min(reach, total - 1) + 1)
        return jnp.stack([one, total - one])
    tallies = jnp.asarray(profile(number_of, total, reach, lean), jnp.int32)
    twos = (number_of - 1) // 2
    giver, taker = tallies[1:1 + 2 * twos:2], tallies[2:2 + 2 * twos:2]
    room = jnp.minimum(giver - 1, reach - taker)
    passed = jax.random.randint(jax.random.fold_in(key, 1), (twos,), 0, 1 << 20) % (room + 1)
    tallies = tallies.at[1:1 + 2 * twos:2].set(giver - passed).at[2:2 + 2 * twos:2].set(taker + passed)
    return tallies[jax.random.permutation(jax.random.fold_in(key, 2), number_of)]


def scatter_about(stream_key, shape, spread, reach, cuts=(), held_as=jnp.bfloat16):
    drawn = jax.random.normal(stream_key, shape, jnp.float32) * spread
    if len(cuts) > 0:
        drawn = level_of(stream_key, shape, cuts, -0.22, 0.18) * drawn
    return jnp.clip(drawn, min=-reach, max=reach).astype(held_as)


def setup_inputs(seed: int = 0, part: int = 0) -> dict:
    key_of = jax.random.split(jax.random.key(seed), 15)
    part_keys = jax.random.split(jax.random.fold_in(key_of[14], part), 15)
    return {
        "qkv": draw_qkv(jax.random.fold_in(jax.random.fold_in(key_of[14], part), 71), part),
        "stream": scatter_about(part_keys[1], (N_SECTION, TOKS, D), 1.0, 6.0, ((0, 2), (1, 8))),
        "out_weight": scatter_about(key_of[2], (HEADS * HD, D), (HEADS * HD) ** -0.5, 0.125, ((0, 2),)),
        "mod_scale": scatter_about(part_keys[3], (N_SECTION, D), 0.5, 3.0, ((0, 2),), jnp.float32),
        "mod_shift": scatter_about(part_keys[4], (N_SECTION, D), 0.5, 3.0, ((0, 2),), jnp.float32),
        "final_weight": scatter_about(key_of[5], (D, PATCH), D ** -0.5, 0.109375),
        "latent": scatter_about(part_keys[6], (N_SECTION, TOKS, PATCH), 1.0, 6.0, ((0, 2), (1, 8)), jnp.float32),
        "step_size": jnp.clip(0.2 + 0.8 * jax.random.uniform(part_keys[7], (N_SECTION,), jnp.float32) ** level_of(part_keys[7], (N_SECTION,), ((0, 2),), -0.2, 0.2), 0.2, 1.0),
        "frame_counts": jax.vmap(lambda own: uneven_parts(own, REQ, FRAMES, MAXF, 2))(jax.random.split(part_keys[8], N_SECTION)).reshape((N_SECTION, REQ)).astype(jnp.int32),
        "finished": with_ends((jax.random.randint(part_keys[9], (N_SECTION, REQ), 0, 2) < 1).astype(jnp.int32), jax.random.fold_in(part_keys[9], 1), 0, 1),
        "conv_weight": scatter_about(key_of[10], (3, 3, 3, LATC, VAEC), (27 * LATC) ** -0.5, 0.3125, ((4, 2),)),
        "conv_bias": scatter_about(key_of[11], (VAEC,), 0.5, 3.0, ((0, 2),), jnp.float32),
        "up_weight": scatter_about(key_of[12], (VAEC, UPC), VAEC ** -0.5, 0.25, ((0, 2),)),
        "up_bias": scatter_about(key_of[13], (UPC,), 0.5, 3.0, ((0, 2),), jnp.float32),
    }


EPSILON = 1e-06

def request_index(positions, counts, unit):
    ends = jnp.cumsum(counts) * unit
    return lax.optimization_barrier(jnp.sum((positions[:, None] >= ends[None, :]).astype(jnp.int32), axis=1))

def attend_section(packed, requests):
    tokens = packed.shape[0]
    block = math.gcd(tokens, 512)
    score_scale = 1.0 / math.sqrt(HD)
    query_heads = jnp.moveaxis(packed[:, 0], 1, 0)
    key_heads = jnp.moveaxis(packed[:, 1], 1, 0)
    value_heads = jnp.moveaxis(packed[:, 2], 1, 0)

    def head_attention(head_trio):
        queries, key_rows, value_rows = head_trio

        def block_attention(block_pair):
            query_rows, query_req = block_pair
            scores = jnp.dot(query_rows, key_rows.T, preferred_element_type=jnp.float32) * score_scale
            allowed = query_req[:, None] == requests[None, :]
            largest = lax.optimization_barrier(jnp.max(jnp.where(allowed, scores, -jnp.inf), axis=1))
            weights = jnp.where(allowed, jnp.exp(scores - largest[:, None]), 0.0)
            weight_sum = lax.optimization_barrier(jnp.sum(weights, axis=1))
            product = jnp.dot(weights.astype(jnp.bfloat16), value_rows, preferred_element_type=jnp.float32)
            return (product / weight_sum[:, None]).astype(jnp.bfloat16)
        blocks = lax.map(block_attention, (queries.reshape(-1, block, HD), requests.reshape(-1, block)))
        return blocks.reshape(tokens, HD)
    heads = lax.map(head_attention, (query_heads, key_heads, value_heads))
    return jnp.moveaxis(heads, 0, 1).reshape(tokens, HEADS * HD)

def decode_frames(frames_video, counts, done_flags, conv_weight, conv_bias, up_weight, up_bias):
    frame_ids = jnp.arange(FRAMES, dtype=jnp.int32)
    owner_req = request_index(frame_ids, counts, 1)
    starts = jnp.cumsum(counts) - counts
    selector = owner_req[:, None] == jnp.arange(REQ, dtype=jnp.int32)[None, :]
    first_frame = lax.optimization_barrier(jnp.sum(jnp.where(selector, starts[None, :], 0), axis=1))
    alive_frame = lax.optimization_barrier(jnp.sum(jnp.where(selector, done_flags[None, :], 0), axis=1))
    padded = jnp.pad(frames_video, ((2, 0), (1, 1), (1, 1), (0, 0)))
    columns_list = []
    for time_tap in range(3):
        inside = frame_ids - 2 + time_tap >= first_frame
        for row_tap in range(3):
            for col_tap in range(3):
                window = padded[time_tap:time_tap + FRAMES, row_tap:row_tap + LROWS, col_tap:col_tap + LCOLS]
                columns_list.append(jnp.where(inside[:, None, None, None], window, jnp.zeros_like(window)))
    stacked = jnp.concatenate(columns_list, axis=3).reshape(-1, 27 * LATC)
    kernel = conv_weight.reshape(27 * LATC, VAEC)
    hidden = jax.nn.silu(jnp.dot(stacked, kernel, preferred_element_type=jnp.float32) + conv_bias).astype(jnp.bfloat16)
    upsampled = jnp.dot(hidden, up_weight, preferred_element_type=jnp.float32) + up_bias
    upsampled = upsampled.reshape(FRAMES, LROWS, LCOLS, UPC) * alive_frame.astype(jnp.float32)[:, None, None, None]
    return upsampled.astype(jnp.bfloat16)

def reference(qkv, stream, out_weight, mod_scale, mod_shift, final_weight, latent, step_size, frame_counts, finished, conv_weight, conv_bias, up_weight, up_bias):
    positions = jnp.arange(TOKS, dtype=jnp.int32)
    latent_list = []
    video_list = []
    for section_index in range(N_SECTION):
        counts = frame_counts[section_index]
        requests = request_index(positions // F_TOK, counts, 1)
        packed = qkv[section_index].reshape(TOKS, 3, HEADS, HD)
        attended = attend_section(packed, requests)
        mixed_stream = stream[section_index].astype(jnp.float32) + jnp.dot(attended, out_weight, preferred_element_type=jnp.float32)
        average = lax.optimization_barrier(jnp.mean(mixed_stream, axis=1, keepdims=True))
        centred = mixed_stream - average
        variance = lax.optimization_barrier(jnp.mean(centred * centred, axis=1, keepdims=True))
        normed = centred / jnp.sqrt(variance + EPSILON)
        modulated = (normed * (1.0 + mod_scale[section_index]) + mod_shift[section_index]).astype(jnp.bfloat16)
        velocity = jnp.dot(modulated, final_weight, preferred_element_type=jnp.float32)
        updated = latent[section_index] + step_size[section_index] * velocity
        latent_list.append(updated)
        frames_video = updated.reshape(FRAMES, PROWS, PCOLS, 2, 2, LATC).transpose(0, 1, 3, 2, 4, 5)
        frames_video = frames_video.reshape(FRAMES, LROWS, LCOLS, LATC).astype(jnp.bfloat16)
        video_list.append(decode_frames(frames_video, counts, finished[section_index], conv_weight, conv_bias, up_weight, up_bias))
    return (jnp.stack(latent_list), jnp.stack(video_list))
```

```python
import math

import jax
import jax.numpy as jnp
from jax import lax
from jax.experimental import pallas as pl
from jax.experimental.pallas import tpu as pltpu
from jax.sharding import PartitionSpec as P

HEADS = 16
HD = 128
LATC = 16
PROWS = 8
PCOLS = 16
F_TOK = 128
LROWS = 16
LCOLS = 32


EPSILON = 1e-06
NEG_FILL = -1e30


def padded_2(value, sides, width):
    for axis, dim in sides:
        peers, length = (lax.axis_size(axis), value.shape[dim])
        up = [(i, (i + 1) % peers) for i in range(peers - 1)]
        down = [(j, i) for i, j in up]
        last = lax.slice_in_dim(value, length - width, length, axis=dim)
        initial = lax.slice_in_dim(value, 0, width, axis=dim)
        before = lax.ppermute(last, axis, up)
        after = lax.ppermute(initial, axis, down)
        value = jnp.concatenate([before, value, after], axis=dim)
    return value


def request_index(positions, counts, unit):
    ends = jnp.cumsum(counts) * unit
    return jnp.sum((positions[:, None] >= ends[None, :]).astype(jnp.int32), axis=1)


def attend_block(running, queries, query_req, key_rows, value_rows, key_req):
    running_max, weight_sum, accumulated = running
    scores = jnp.einsum("qhd,khd->qhk", queries, key_rows, preferred_element_type=jnp.float32) * (
        1.0 / math.sqrt(queries.shape[2])
    )
    allowed = (query_req[:, None] == key_req[None, :])[:, None, :]
    masked = jnp.where(allowed, scores, NEG_FILL)
    new_max = jnp.maximum(running_max, jnp.max(masked, axis=2))
    weights = jnp.where(allowed, jnp.exp(masked - new_max[:, :, None]), 0.0)
    factor = jnp.exp(running_max - new_max)
    weight_sum = weight_sum * factor + jnp.sum(weights, axis=2)
    product = jnp.einsum(
        "qhk,khd->qhd", weights.astype(jnp.bfloat16), value_rows, preferred_element_type=jnp.float32
    )
    accumulated = accumulated * factor[:, :, None] + product
    return (new_max, weight_sum, accumulated)


def fold_keys(running, queries, query_req, key_rows, value_rows, key_req):
    row_count = key_rows.shape[0]
    lowest = jnp.min(query_req)
    highest = jnp.max(query_req)

    def key_block(folded, block_data):
        block_keys, block_values, block_req = block_data
        touches = jnp.logical_and(jnp.min(block_req) <= highest, jnp.max(block_req) >= lowest)
        result = lax.cond(
            touches,
            lambda current: attend_block(
                current, queries, query_req, block_keys, block_values, block_req
            ),
            lambda current: current,
            folded,
        )
        return (result, None)

    pieces = row_count // 512
    shaped_keys = key_rows.reshape(pieces, 512, key_rows.shape[1], key_rows.shape[2])
    shaped_values = value_rows.reshape(pieces, 512, value_rows.shape[1], value_rows.shape[2])
    shaped_req = key_req.reshape(pieces, 512)
    folded, _ = lax.scan(key_block, running, (shaped_keys, shaped_values, shaped_req))
    return folded


def empty_state(queries):
    query_rows, heads_here, head_size = queries.shape
    return (
        jnp.full((query_rows, heads_here), NEG_FILL, jnp.float32),
        jnp.zeros((query_rows, heads_here), jnp.float32),
        jnp.zeros((query_rows, heads_here, head_size), jnp.float32),
    )


def normalize(folded):
    return (folded[2] / folded[1][:, :, None]).astype(jnp.bfloat16)


def on_device(
    qkv,
    stream,
    out_weight,
    mod_scale,
    mod_shift,
    final_weight,
    latent,
    step_size,
    frame_counts,
    finished,
    conv_weight,
    conv_bias,
    up_weight,
    up_bias,
):
    tp_count = lax.axis_size("tp")
    tp_place = lax.axis_index("tp")
    token_rows = qkv.shape[1]
    counts = frame_counts[0]
    done_flags = finished[0]
    packed = qkv[0].reshape(token_rows, 3, HEADS, HD)
    regrouped = lax.all_to_all(packed, "seq", split_axis=2, concat_axis=0, tiled=True)
    local_rows = regrouped.shape[0]
    positions = jnp.arange(local_rows, dtype=jnp.int32)
    token_queries = (
        positions // token_rows * tp_count + tp_place
    ) * token_rows + positions % token_rows
    query_req = request_index(token_queries // F_TOK, counts, 1)
    queries = regrouped[:, 0]
    key_portion = (
        lax.all_gather(regrouped[:, 1], "tp", axis=0, tiled=True),
        lax.all_gather(regrouped[:, 2], "tp", axis=0, tiled=True),
    )
    key_index = jnp.arange(key_portion[0].shape[0], dtype=jnp.int32)
    source = key_index // local_rows
    within = key_index % local_rows
    key_tokens = (within // token_rows * tp_count + source) * token_rows + within % token_rows
    folded = fold_keys(
        empty_state(queries),
        queries,
        query_req,
        key_portion[0],
        key_portion[1],
        request_index(key_tokens // F_TOK, counts, 1),
    )
    returned = lax.all_to_all(
        lax.all_to_all(normalize(folded), "seq", split_axis=0, concat_axis=1, tiled=True),
        "tp",
        split_axis=1,
        concat_axis=0,
        tiled=True,
    )
    flattened = returned.reshape(returned.shape[0], returned.shape[1] * returned.shape[2])
    summed = lax.psum_scatter(
        jnp.dot(flattened, out_weight, preferred_element_type=jnp.float32).astype(jnp.bfloat16),
        "tp",
        scatter_dimension=0,
        tiled=True,
    ).astype(jnp.float32)
    mixed_stream = stream[0].astype(jnp.float32) + summed
    average = jnp.mean(mixed_stream, axis=1, keepdims=True)
    centred = mixed_stream - average
    variance = jnp.mean(centred * centred, axis=1, keepdims=True)
    normed = centred / jnp.sqrt(variance + EPSILON)
    modulated = (normed * (1.0 + mod_scale[0]) + mod_shift[0]).astype(jnp.bfloat16)
    velocity = jnp.dot(modulated, final_weight, preferred_element_type=jnp.float32)
    updated = latent[0] + step_size[0] * velocity
    frame_local = token_rows // F_TOK
    own_video = updated.reshape(frame_local, PROWS, PCOLS, 2, 2, LATC).transpose(0, 1, 3, 2, 4, 5)
    own_video = own_video.reshape(frame_local, LROWS, LCOLS, LATC).astype(jnp.bfloat16)
    matched_pairs = lax.all_gather(own_video, "tp", axis=0, tiled=True)
    slab_grouped = lax.all_to_all(matched_pairs, "seq", split_axis=1, concat_axis=0, tiled=True)
    frame_count_total = slab_grouped.shape[0]
    rows_per_slab = slab_grouped.shape[1]
    with_halo_rows = padded_2(slab_grouped, (("seq", 1),), 1)
    padded = jnp.pad(with_halo_rows, ((2, 0), (0, 0), (1, 1), (0, 0)))
    frame_ids = jnp.arange(frame_count_total, dtype=jnp.int32)
    owner_req = request_index(frame_ids, counts, 1)
    starts = jnp.cumsum(counts) - counts
    selector = owner_req[:, None] == jnp.arange(counts.shape[0], dtype=jnp.int32)[None, :]
    first_frame = jnp.sum(jnp.where(selector, starts[None, :], 0), axis=1)
    alive_frame = jnp.sum(jnp.where(selector, done_flags[None, :], 0), axis=1)
    columns_list = []
    for time_tap in range(3):
        inside = frame_ids - 2 + time_tap >= first_frame
        for row_tap in range(3):
            for col_tap in range(3):
                window = padded[
                    time_tap : time_tap + frame_count_total,
                    row_tap : row_tap + rows_per_slab,
                    col_tap : col_tap + LCOLS,
                ]
                columns_list.append(
                    jnp.where(inside[:, None, None, None], window, jnp.zeros_like(window))
                )
    stacked = jnp.concatenate(columns_list, axis=3).reshape(-1, 27 * LATC)
    whole_kernel, whole_bias = (
        lax.all_gather(
            conv_weight.astype(jnp.float32).astype(jnp.bfloat16), "tp", axis=4, tiled=True
        ).astype(jnp.float32),
        lax.all_gather(conv_bias.astype(jnp.bfloat16), "tp", axis=0, tiled=True).astype(
            conv_bias.dtype
        ),
    )
    kernel = whole_kernel.astype(jnp.bfloat16).reshape(27 * LATC, whole_kernel.shape[4])
    hidden = jax.nn.silu(
        jnp.dot(stacked, kernel, preferred_element_type=jnp.float32) + whole_bias
    ).astype(jnp.bfloat16)
    own_columns = lax.all_to_all(up_weight, "tp", split_axis=1, concat_axis=0, tiled=True)
    shared = jnp.dot(hidden, own_columns, preferred_element_type=jnp.float32).reshape(
        frame_count_total, rows_per_slab, LCOLS, own_columns.shape[1]
    )
    decoded = ((shared + up_bias) * alive_frame.astype(jnp.float32)[:, None, None, None]).astype(
        jnp.bfloat16
    )
    return (updated[None], decoded[None])


NN = (((1,), (0,)), ((), ()))
NT = (((1,), (1,)), ((), ()))


def request_of(frame, ends):
    owner = (frame >= ends[0]).astype(jnp.int32)
    for end in ends[1:]:
        owner = owner + (frame >= end).astype(jnp.int32)
    return owner


def frame_ends(counts_ref, requests):
    ends = [counts_ref[0, 0]]
    for i in range(1, requests):
        ends.append(ends[-1] + counts_ref[0, i])
    return ends


def slab_start(seq, rows):
    return jnp.clip(seq * rows - 1, 0, PROWS - rows - 2)


def expand_weight(kernel_ref, expanded_ref, patch):
    for i in range(2):
        for j in range(2):
            for a in range(3):
                for dr in range(2):
                    for dc in range(2):
                        for i2 in range(2):
                            for j2 in range(2):
                                b = i - 1 + 2 * dr + i2
                                e = j - 1 + 2 * dc + j2
                                if 0 <= b < 3 and 0 <= e < 3:
                                    to = ((a * 2 + dr) * 2 + dc) * patch + (i2 * 2 + j2) * LATC
                                    come = ((a * 3 + b) * 3 + e) * LATC
                                    expanded_ref[i * 2 + j, to : to + LATC] = kernel_ref[come : come + LATC]


def attend_kernel(
    n,
    window,
    requests,
    qkv_ref,
    stream_ref,
    ow_ref,
    scale_hbm,
    shift_hbm,
    fw_hbm,
    latent_hbm,
    step_hbm,
    counts_hbm,
    finished_hbm,
    cw_ref,
    cb_ref,
    uw_ref,
    ub_hbm,
    new_latent_ref,
    decoded_ref,
    video_ref,
    expanded_ref,
    cb2_ref,
    uw2_ref,
    ub_ref,
    shifted,
    columns,
    spread,
    qkv_buf,
    cw2_ref,
    scale_ref,
    shift_ref,
    fw_ref,
    latent_ref,
    step_ref,
    counts_ref,
    finished_ref,
    q_buf,
    kv_buf,
    w_buf,
    stream_buf,
    bias_buf,
    max_buf,
    sum_buf,
    acc_buf,
    att_buf,
    part_buf,
    got_buf,
    mixed_buf,
    own_video,
    local_sems,
    q_sems,
    kv_send,
    kv_recv,
    part_send,
    part_recv,
    wt_send,
    wt_recv,
    vid_send,
    vid_recv,
):
    s = lax.axis_index("seq")
    t = lax.axis_index("tp")
    o = 1 - t
    me = s * 2 + t
    devices = 2 * n
    half = q_buf.shape[2]
    heads = half // HD
    hops = (window + 1) // 2
    out_half = uw_ref.shape[1] // 2
    ccols = cw_ref.shape[1]

    def at(seq, tp):
        return {"seq": seq, "tp": tp}

    def remote(src, dst, send, recv, target):
        return pltpu.make_async_remote_copy(
            src_ref=src,
            dst_ref=dst,
            send_sem=send,
            recv_sem=recv,
            device_id=target,
            device_id_type=pl.DeviceIdType.MESH,
        )

    def peer_of(k):
        peer = lax.rem(me + k, devices)
        return at(peer // 2, lax.rem(peer, 2))

    def cols(which, width):
        return pl.ds(pl.multiple_of(which * width, width), width)

    own_q = pltpu.make_async_copy(qkv_ref.at[0, :, cols(t, half)], q_buf.at[1], local_sems.at[0])
    own_kv = pltpu.make_async_copy(
        qkv_ref.at[1:3, :, cols(t, half)], kv_buf.at[window + t], local_sems.at[1]
    )
    get_w = pltpu.make_async_copy(ow_ref, w_buf, local_sems.at[2])
    get_stream = pltpu.make_async_copy(stream_ref, stream_buf, local_sems.at[3])
    stage = pltpu.make_async_copy(qkv_ref, qkv_buf, local_sems.at[13])
    get_counts = pltpu.make_async_copy(counts_hbm, counts_ref, local_sems.at[14])
    get_finished = pltpu.make_async_copy(finished_hbm, finished_ref, local_sems.at[15])
    stage.start()
    get_counts.start()
    get_finished.start()
    own_q.start()
    own_kv.start()

    barrier = pltpu.get_barrier_semaphore()
    for k in range(1, devices):
        pl.semaphore_signal(
            barrier, inc=1, device_id=peer_of(k), device_id_type=pl.DeviceIdType.MESH
        )
    pl.semaphore_wait(barrier, devices - 1)
    stage.wait()
    get_counts.wait()
    get_finished.wait()

    def kv_copy(target_tp, target_seq, slot, send):
        return remote(
            qkv_buf.at[1:3, :, cols(target_tp, half)],
            kv_buf.at[slot],
            kv_send.at[send],
            kv_recv.at[slot],
            at(target_seq, target_tp),
        )

    has_left = s > 0
    has_right = s < n - 1
    rights = [kv_copy(k, s + 1, window + t - 2, k) for k in range(2)]
    lefts = [kv_copy(k, s - 1, window + t + 2, 2 + k) for k in range(2)]
    partner_q = remote(
        qkv_buf.at[0, :, cols(o, half)], q_buf.at[0], q_sems.at[0], q_sems.at[1], at(s, o)
    )
    partner_kv = kv_copy(o, s, window + t, 4)

    @pl.when(has_right)
    def _():
        for copy in rights:
            copy.start()

    @pl.when(has_left)
    def _():
        for copy in lefts:
            copy.start()

    partner_q.start()
    partner_kv.start()
    give_cw = remote(cw_ref, cw2_ref.at[:, ccols:], wt_send.at[0], wt_recv.at[0], at(s, o))
    give_cb = remote(cb_ref, cb2_ref.at[:, ccols:], wt_send.at[1], wt_recv.at[1], at(s, o))
    give_uw = remote(
        uw_ref.at[:, cols(o, out_half)],
        uw2_ref.at[pl.ds(uw_ref.shape[0], uw_ref.shape[0])],
        wt_send.at[2],
        wt_recv.at[2],
        at(s, o),
    )
    give_cw.start()
    give_cb.start()
    give_uw.start()
    loads = [
        pltpu.make_async_copy(source, target, local_sems.at[4 + i])
        for i, (source, target) in enumerate(
            (
                (cw_ref, cw2_ref.at[:, :ccols]),
                (cb_ref, cb2_ref.at[:, :ccols]),
                (uw_ref.at[:, cols(t, out_half)], uw2_ref.at[: uw_ref.shape[0]]),
                (scale_hbm, scale_ref),
                (shift_hbm, shift_ref),
                (fw_hbm, fw_ref),
                (latent_hbm, latent_ref),
                (step_hbm, step_ref),
                (ub_hbm, ub_ref),
            )
        )
    ]
    for load in loads:
        load.start()
    get_stream.start()
    get_w.start()

    ends = frame_ends(counts_ref, requests)
    query_req = (request_of(s * 2 + o, ends), request_of(s * 2 + t, ends))
    score_scale = 1.0 / math.sqrt(HD)

    def wait_slot(slot):
        remote(kv_buf.at[slot], kv_buf.at[slot], kv_send.at[0], kv_recv.at[slot], at(s, o)).wait_recv()

    def attend_far(slot, place, query_frame):
        key_req = request_of(s * 2 - window + slot, ends)
        bias = jnp.where(request_of(query_frame, ends) == key_req, 0.0, NEG_FILL).astype(jnp.float32)
        rows = pl.ds(pl.multiple_of(place * F_TOK, F_TOK), F_TOK)

        def one_head(h, carry):
            lanes = pl.ds(pl.multiple_of(h * HD, HD), HD)
            q = q_buf[place, :, lanes]
            scores = lax.dot_general(
                q, kv_buf[slot, 0, :, lanes], NT, preferred_element_type=jnp.float32
            )
            scores = scores * score_scale + bias
            old = max_buf[h, rows, :]
            top = jnp.maximum(old, jnp.max(scores, axis=1, keepdims=True))
            weights = jnp.exp(scores - top)
            factor = jnp.exp(old - top)
            sum_buf[h, rows, :] = sum_buf[h, rows, :] * factor + jnp.sum(
                weights, axis=1, keepdims=True
            )
            acc_buf[h, rows, :] = acc_buf[h, rows, :] * factor + lax.dot_general(
                weights.astype(jnp.bfloat16),
                kv_buf[slot, 1, :, lanes],
                NN,
                preferred_element_type=jnp.float32,
            )
            return carry

        lax.fori_loop(0, heads, one_head, 0, unroll=True)

    def attend(first, width, fresh):
        for i in range(2):
            for j in range(width):
                key_req = request_of(s * 2 - window + first + j, ends)
                bias = jnp.where(query_req[i] == key_req, 0.0, NEG_FILL).astype(jnp.float32)
                bias_buf[pl.ds(i * F_TOK, F_TOK), pl.ds(j * F_TOK, F_TOK)] = jnp.full(
                    (F_TOK, F_TOK), bias, jnp.float32
                )
        bias = bias_buf[:, : width * F_TOK]

        def one_head(h, carry):
            lanes = pl.ds(pl.multiple_of(h * HD, HD), HD)
            q = q_buf[:, :, lanes].reshape(2 * F_TOK, HD)
            keys = kv_buf[first : first + width, 0, :, lanes].reshape(width * F_TOK, HD)
            values = kv_buf[first : first + width, 1, :, lanes].reshape(width * F_TOK, HD)
            scores = lax.dot_general(q, keys, NT, preferred_element_type=jnp.float32)
            scores = scores * score_scale + bias
            top = jnp.max(scores, axis=1, keepdims=True)
            if not fresh:
                old = max_buf[h]
                top = jnp.maximum(old[:, :1], top)
            weights = jnp.exp(scores - top)
            total = jnp.sum(weights, axis=1, keepdims=True)
            product = lax.dot_general(
                weights.astype(jnp.bfloat16), values, NN, preferred_element_type=jnp.float32
            )
            if not fresh:
                factor = jnp.exp(old[:, :1] - top)
                total = total + sum_buf[h][:, :1] * factor
                product = product + acc_buf[h] * factor
            max_buf[h] = jnp.broadcast_to(top, (2 * F_TOK, HD))
            sum_buf[h] = jnp.broadcast_to(total, (2 * F_TOK, HD))
            acc_buf[h] = product
            return carry

        lax.fori_loop(0, heads, one_head, 0, unroll=4)

    own_q.wait()
    own_kv.wait()
    partner_q.wait_recv()
    wait_slot(window + o)
    attend(window, 2, True)

    loads[0].wait()
    give_cw.wait()
    expanded_ref[...] = jnp.zeros_like(expanded_ref)
    expand_weight(cw2_ref, expanded_ref, new_latent_ref.shape[0])

    relays = []
    for d in range(1, hops + 1):
        low = window - 2 * d
        high = window + 2 * d
        two = 2 * d <= window
        more = d < hops

        def receive(first, width, good, forward, good_next, step, base, sends):
            @pl.when(good)
            def _():
                for j in range(width):
                    wait_slot(first + j)

            copies = []
            if forward:
                for slot in forward:
                    copies.append(
                        remote(
                            kv_buf.at[slot],
                            kv_buf.at[slot - 2 * step],
                            kv_send.at[sends + len(copies)],
                            kv_recv.at[slot - 2 * step],
                            at(s + step, t),
                        )
                    )

                @pl.when(good_next)
                def _():
                    for copy in copies:
                        copy.start()

            return [(copy, good_next) for copy in copies]

        base = 5 + 4 * (d - 1)
        wide = 2 if two else 1
        next_two = 2 * (d + 1) <= window
        left_first = low if two else low + 1
        left_good = s >= d
        right_good = s <= n - 1 - d
        left_fwd = ([low, low + 1] if next_two else [low + 1]) if more else []
        right_fwd = ([high, high + 1] if next_two else [high]) if more else []
        def attend_left():
            @pl.when(left_good)
            def _():
                if two:
                    attend(left_first, 2, False)
                else:
                    attend_far(left_first, o, s * 2)

        relays += receive(
            left_first, wide, left_good, left_fwd, jnp.logical_and(left_good, has_right), 1, d, base
        )
        if not more:
            attend_left()
        relays += receive(
            high, wide, right_good, right_fwd, jnp.logical_and(right_good, has_left), -1, d, base + 2
        )
        if more:
            attend_left()

        @pl.when(right_good)
        def _():
            if two:
                attend(high, 2, False)
            else:
                attend_far(high, t, s * 2 + 1)

    for h in range(heads):
        att_buf[:, h * HD : (h + 1) * HD] = (acc_buf[h] / sum_buf[h]).astype(jnp.bfloat16)

    get_w.wait()
    get_stream.wait()
    for load in loads[1:]:
        load.wait()
    chunks, _, chunk = part_buf.shape
    attended = att_buf[...]
    parts = []
    for c in range(chunks):
        span = pl.ds(c * chunk, chunk)
        result = lax.dot_general(attended, w_buf[:, span], NN, preferred_element_type=jnp.float32)
        part_buf[c] = result[:F_TOK].astype(jnp.bfloat16)
        copy = remote(part_buf.at[c], got_buf.at[c], part_send.at[c], part_recv.at[c], at(s, o))
        copy.start()
        parts.append(copy)
        mixed_buf[:, span] = result[F_TOK:] + stream_buf[:, span].astype(jnp.float32)
    row_sum = jnp.zeros((F_TOK, 1), jnp.float32)
    for c in range(chunks):
        span = pl.ds(c * chunk, chunk)
        parts[c].wait_recv()
        mixed = mixed_buf[:, span] + got_buf[c].astype(jnp.float32)
        mixed_buf[:, span] = mixed
        row_sum = row_sum + jnp.sum(mixed, axis=1, keepdims=True)
    width = mixed_buf.shape[1]
    average = row_sum / width
    row_square = jnp.zeros((F_TOK, 1), jnp.float32)
    for c in range(chunks):
        centred = mixed_buf[:, c * chunk : (c + 1) * chunk] - average
        row_square = row_square + jnp.sum(centred * centred, axis=1, keepdims=True)
    inverse = 1.0 / jnp.sqrt(row_square / width + EPSILON)
    velocity = jnp.zeros((fw_ref.shape[0], F_TOK), jnp.float32)
    for c in range(chunks):
        span = pl.ds(c * chunk, chunk)
        normed = (mixed_buf[:, span] - average) * inverse
        modulated = (normed * (1.0 + scale_ref[:, span]) + shift_ref[:, span]).astype(jnp.bfloat16)
        velocity = velocity + lax.dot_general(
            fw_ref[:, span], modulated, NT, preferred_element_type=jnp.float32
        )
    updated = latent_ref[...] + step_ref[0, 0] * velocity
    new_latent_ref[...] = updated
    own_video[...] = updated.T.astype(jnp.bfloat16)
    kept = video_ref.shape[1]

    def needed(seq):
        first = slab_start(seq, kept // PCOLS - 2) * PCOLS
        return pl.ds(pl.multiple_of(first, PCOLS), kept)

    sends = []
    for k in range(1, devices):
        target = peer_of(k)
        copy = remote(
            own_video.at[needed(target["seq"])],
            video_ref.at[me],
            vid_send.at[k - 1],
            vid_recv.at[k - 1],
            target,
        )
        copy.start()
        sends.append(copy)
    video_ref[me] = own_video[needed(s), :]

    partner_q.wait_send()
    partner_kv.wait_send()

    @pl.when(has_right)
    def _():
        for copy in rights:
            copy.wait_send()

    @pl.when(has_left)
    def _():
        for copy in lefts:
            copy.wait_send()

    for copy, good in relays:

        @pl.when(good)
        def _(copy=copy):
            copy.wait_send()

    for copy in parts:
        copy.wait_send()
    give_cb.wait()
    give_uw.wait()
    for copy in sends:
        copy.wait()
    decode_frames(
        kept // PCOLS - 2,
        requests,
        video_ref,
        expanded_ref,
        cb2_ref,
        uw2_ref,
        ub_ref,
        counts_ref,
        finished_ref,
        decoded_ref,
        shifted,
        columns,
        spread,
    )


def decode_frames(
    rows,
    requests,
    video_ref,
    expanded,
    cb_ref,
    uw_ref,
    ub_ref,
    counts_ref,
    finished_ref,
    out_ref,
    shifted,
    columns,
    spread,
):
    s = lax.axis_index("seq")
    frames = video_ref.shape[0]
    group = rows + 2
    span = group * PCOLS
    patch = video_ref.shape[2]
    ends = frame_ends(counts_ref, requests)
    owners = [request_of(jnp.int32(f), ends) for f in range(frames)]

    pieces = []
    for f in range(frames):
        for r in range(group):
            row = s * rows + r - 1
            inside = jnp.logical_and(row >= 0, row < PROWS)
            clamped = jnp.clip(row, 0, PROWS - 1) - slab_start(s, rows)
            piece = video_ref[f, pl.ds(pl.multiple_of(clamped * PCOLS, PCOLS), PCOLS), :]
            pieces.append(jnp.where(inside, piece.astype(jnp.float32), 0.0))
    middle = jnp.concatenate(pieces, axis=0)
    total = frames * span
    column = lax.rem(lax.broadcasted_iota(jnp.int32, (total, patch), 0), PCOLS)
    before = jnp.where(column == 0, 0.0, pltpu.roll(middle, 1, 0))
    after = jnp.where(column == PCOLS - 1, 0.0, pltpu.roll(middle, total - 1, 0))
    shifted[0] = jnp.concatenate([before, middle], axis=1).astype(jnp.bfloat16)
    shifted[1] = jnp.concatenate([middle, after], axis=1).astype(jnp.bfloat16)

    block = rows * PCOLS
    lanes = 2 * patch
    for f in range(frames):
        for a in range(3):
            g = f - 2 + a
            for i in range(2):
                for dr in range(2):
                    for j in range(2):
                        place = pl.ds((a * 2 + dr) * lanes, lanes)
                        if g < 0:
                            value = jnp.zeros((block, lanes), jnp.bfloat16)
                        else:
                            first = g * span + (i + dr) * PCOLS
                            value = shifted[j, first : first + block]
                            if g != f:
                                keep = (owners[g] == owners[f]).astype(jnp.float32)
                                value = value * jnp.full((1, lanes), keep, jnp.float32).astype(
                                    jnp.bfloat16
                                )
                        columns[i * 2 + j, f * block : (f + 1) * block, place] = value

    alive = []
    for f in range(frames):
        flag = jnp.float32(0)
        for r in range(requests):
            flag = flag + jnp.where(owners[f] == r, finished_ref[0, r], 0).astype(jnp.float32)
        alive.append(flag)
    out_cols = uw_ref.shape[1]
    for i in range(2):
        for j in range(2):
            hidden = lax.dot_general(
                columns[i * 2 + j], expanded[i * 2 + j], NN, preferred_element_type=jnp.float32
            )
            hidden = jax.nn.silu(hidden + cb_ref[...]).astype(jnp.bfloat16)
            shared = lax.dot_general(hidden, uw_ref[...], NN, preferred_element_type=jnp.float32)
            shared = shared + ub_ref[...]
            for f in range(frames):
                for r in range(rows):
                    first = f * block + r * PCOLS
                    value = shared[first : first + PCOLS] * alive[f]
                    for c in range(out_cols // 128):
                        spread[c, f, 2 * r + i, pl.ds(j, PCOLS, stride=2), :] = value[
                            :, c * 128 : (c + 1) * 128
                        ]
    for c in range(out_cols // 128):
        out_ref[:, :, :, c * 128 : (c + 1) * 128] = spread[c].astype(jnp.bfloat16)


def on_device_fast(
    qkv,
    stream,
    out_weight,
    mod_scale,
    mod_shift,
    final_weight,
    latent,
    step_size,
    frame_counts,
    finished,
    conv_weight,
    conv_bias,
    up_weight,
    up_bias,
):
    n = lax.axis_size("seq")
    frames = 2 * n
    window = frames // 2 - 1
    requests = frame_counts.shape[1]
    width = stream.shape[2]
    patch = latent.shape[2]
    half = out_weight.shape[0]
    heads = half // HD
    ccols = conv_weight.shape[4]
    taps = conv_weight.shape[0] * conv_weight.shape[1] * conv_weight.shape[2] * LATC
    up_rows, up_all = up_weight.shape
    out_half = up_all // 2
    slots = 2 * window + 2
    hops = (window + 1) // 2
    rows = PROWS // n
    chunks = 6
    chunk = width // chunks
    vmem = pl.BlockSpec(memory_space=pltpu.VMEM)
    anyspace = pl.BlockSpec(memory_space=pltpu.HBM)
    bf16, f32 = jnp.bfloat16, jnp.float32
    dma = pltpu.SemaphoreType.DMA
    new_latent, decoded = pl.pallas_call(
        lambda *refs: attend_kernel(n, window, requests, *refs),
        name="attend",
        out_shape=(
            jax.ShapeDtypeStruct((patch, F_TOK), f32),
            jax.ShapeDtypeStruct((frames, 2 * rows, LCOLS, out_half), bf16),
        ),
        in_specs=[
            anyspace,
            anyspace,
            anyspace,
            anyspace,
            anyspace,
            anyspace,
            anyspace,
            anyspace,
            anyspace,
            anyspace,
            anyspace,
            anyspace,
            anyspace,
            anyspace,
        ],
        out_specs=(vmem,) * 2,
        scratch_shapes=[
            pltpu.VMEM((frames, (rows + 2) * PCOLS, patch), bf16),
            pltpu.VMEM((4, 12 * patch, 2 * ccols), bf16),
            pltpu.VMEM((1, 2 * ccols), f32),
            pltpu.VMEM((2 * up_rows, out_half), bf16),
            pltpu.VMEM((1, out_half), f32),
            pltpu.VMEM((2, frames * (rows + 2) * PCOLS, 2 * patch), bf16),
            pltpu.VMEM((4, frames * rows * PCOLS, 12 * patch), bf16),
            pltpu.VMEM((out_half // 128, frames, 2 * rows, LCOLS, 128), f32),
            pltpu.VMEM((3, F_TOK, 2 * half), bf16),
            pltpu.VMEM((taps, 2 * ccols), bf16),
            pltpu.VMEM((1, width), f32),
            pltpu.VMEM((1, width), f32),
            pltpu.VMEM((patch, width), bf16),
            pltpu.VMEM((patch, F_TOK), f32),
            pltpu.SMEM((1, 1), f32),
            pltpu.SMEM((1, requests), jnp.int32),
            pltpu.SMEM((1, requests), jnp.int32),
            pltpu.VMEM((2, F_TOK, half), bf16),
            pltpu.VMEM((slots, 2, F_TOK, half), bf16),
            pltpu.VMEM((half, width), bf16),
            pltpu.VMEM((F_TOK, width), bf16),
            pltpu.VMEM((2 * F_TOK, 2 * F_TOK), f32),
            pltpu.VMEM((heads, 2 * F_TOK, HD), f32),
            pltpu.VMEM((heads, 2 * F_TOK, HD), f32),
            pltpu.VMEM((heads, 2 * F_TOK, HD), f32),
            pltpu.VMEM((2 * F_TOK, half), bf16),
            pltpu.VMEM((chunks, F_TOK, chunk), bf16),
            pltpu.VMEM((chunks, F_TOK, chunk), bf16),
            pltpu.VMEM((F_TOK, width), f32),
            pltpu.VMEM((F_TOK, patch), bf16),
            dma((16,)),
            dma((2,)),
            dma((5 + 4 * hops,)),
            dma((slots,)),
            dma((chunks,)),
            dma((chunks,)),
            dma((3,)),
            dma((3,)),
            dma((2 * n - 1,)),
            dma((2 * n - 1,)),
        ],
        compiler_params=pltpu.CompilerParams(
            collective_id=0, has_side_effects=True, vmem_limit_bytes=41943040
        ),
    )(
        *(
            value if value.size == 1 else pltpu.with_memory_space_constraint(value, pltpu.HBM)
            for value in (
                qkv[0].transpose(1, 0, 2),
                stream[0],
                out_weight,
                mod_scale,
                mod_shift,
                final_weight.T,
                latent[0].T,
                step_size[None],
                frame_counts,
                finished,
                conv_weight.reshape(taps, ccols),
                conv_bias[None],
                up_weight,
                up_bias[None],
            )
        )
    )
    return (new_latent.T[None], decoded[None])


def solution(mesh):
    fast = LROWS // mesh.shape["seq"] % 2 == 0 and mesh.shape["tp"] == 2
    in_specs = (
        P(("groups", "section"), ("seq", "tp"), None, None),
        P(("groups", "section"), ("seq", "tp"), None),
        P("tp", None),
        P(("groups", "section"), None),
        P(("groups", "section"), None),
        P(),
        P(("groups", "section"), ("seq", "tp"), None),
        P(("groups", "section")),
        P(("groups", "section"), None),
        P(("groups", "section"), None),
        P(None, None, None, None, "tp"),
        P("tp"),
        P("tp", None),
        P("tp"),
    )
    out_specs = (
        P(("groups", "section"), ("seq", "tp"), None),
        P(("groups", "section"), None, "seq", None, "tp"),
    )
    return jax.shard_map(
        on_device_fast if fast else on_device, mesh=mesh, in_specs=in_specs, out_specs=out_specs, check_vma=False
    )
```

```python
import math

import jax
import jax.numpy as jnp
from jax import lax
from jax.experimental import pallas as pl
from jax.experimental.pallas import tpu as pltpu
from jax.sharding import PartitionSpec as P

HEADS = 16
HD = 128
LATC = 16
PROWS = 8
PCOLS = 16
F_TOK = 128
LROWS = 16
LCOLS = 32


EPSILON = 1e-06
NEG_FILL = -1e30


def padded_2(value, sides, width):
    for axis, dim in sides:
        peers, length = (lax.axis_size(axis), value.shape[dim])
        up = [(i, (i + 1) % peers) for i in range(peers - 1)]
        down = [(j, i) for i, j in up]
        last = lax.slice_in_dim(value, length - width, length, axis=dim)
        initial = lax.slice_in_dim(value, 0, width, axis=dim)
        before = lax.ppermute(last, axis, up)
        after = lax.ppermute(initial, axis, down)
        value = jnp.concatenate([before, value, after], axis=dim)
    return value


def request_index(positions, counts, unit):
    ends = jnp.cumsum(counts) * unit
    return jnp.sum((positions[:, None] >= ends[None, :]).astype(jnp.int32), axis=1)


def attend_block(running, queries, query_req, key_rows, value_rows, key_req):
    running_max, weight_sum, accumulated = running
    scores = jnp.einsum("qhd,khd->qhk", queries, key_rows, preferred_element_type=jnp.float32) * (
        1.0 / math.sqrt(queries.shape[2])
    )
    allowed = (query_req[:, None] == key_req[None, :])[:, None, :]
    masked = jnp.where(allowed, scores, NEG_FILL)
    new_max = jnp.maximum(running_max, jnp.max(masked, axis=2))
    weights = jnp.where(allowed, jnp.exp(masked - new_max[:, :, None]), 0.0)
    factor = jnp.exp(running_max - new_max)
    weight_sum = weight_sum * factor + jnp.sum(weights, axis=2)
    product = jnp.einsum(
        "qhk,khd->qhd", weights.astype(jnp.bfloat16), value_rows, preferred_element_type=jnp.float32
    )
    accumulated = accumulated * factor[:, :, None] + product
    return (new_max, weight_sum, accumulated)


def fold_keys(running, queries, query_req, key_rows, value_rows, key_req):
    row_count = key_rows.shape[0]
    lowest = jnp.min(query_req)
    highest = jnp.max(query_req)

    def key_block(folded, block_data):
        block_keys, block_values, block_req = block_data
        touches = jnp.logical_and(jnp.min(block_req) <= highest, jnp.max(block_req) >= lowest)
        result = lax.cond(
            touches,
            lambda current: attend_block(
                current, queries, query_req, block_keys, block_values, block_req
            ),
            lambda current: current,
            folded,
        )
        return (result, None)

    pieces = row_count // 512
    shaped_keys = key_rows.reshape(pieces, 512, key_rows.shape[1], key_rows.shape[2])
    shaped_values = value_rows.reshape(pieces, 512, value_rows.shape[1], value_rows.shape[2])
    shaped_req = key_req.reshape(pieces, 512)
    folded, _ = lax.scan(key_block, running, (shaped_keys, shaped_values, shaped_req))
    return folded


def empty_state(queries):
    query_rows, heads_here, head_size = queries.shape
    return (
        jnp.full((query_rows, heads_here), NEG_FILL, jnp.float32),
        jnp.zeros((query_rows, heads_here), jnp.float32),
        jnp.zeros((query_rows, heads_here, head_size), jnp.float32),
    )


def normalize(folded):
    return (folded[2] / folded[1][:, :, None]).astype(jnp.bfloat16)


def on_device(
    qkv,
    stream,
    out_weight,
    mod_scale,
    mod_shift,
    final_weight,
    latent,
    step_size,
    frame_counts,
    finished,
    conv_weight,
    conv_bias,
    up_weight,
    up_bias,
):
    tp_count = lax.axis_size("tp")
    tp_place = lax.axis_index("tp")
    token_rows = qkv.shape[1]
    counts = frame_counts[0]
    done_flags = finished[0]
    packed = qkv[0].reshape(token_rows, 3, HEADS, HD)
    regrouped = lax.all_to_all(packed, "seq", split_axis=2, concat_axis=0, tiled=True)
    local_rows = regrouped.shape[0]
    positions = jnp.arange(local_rows, dtype=jnp.int32)
    token_queries = (
        positions // token_rows * tp_count + tp_place
    ) * token_rows + positions % token_rows
    query_req = request_index(token_queries // F_TOK, counts, 1)
    queries = regrouped[:, 0]
    key_portion = (
        lax.all_gather(regrouped[:, 1], "tp", axis=0, tiled=True),
        lax.all_gather(regrouped[:, 2], "tp", axis=0, tiled=True),
    )
    key_index = jnp.arange(key_portion[0].shape[0], dtype=jnp.int32)
    source = key_index // local_rows
    within = key_index % local_rows
    key_tokens = (within // token_rows * tp_count + source) * token_rows + within % token_rows
    folded = fold_keys(
        empty_state(queries),
        queries,
        query_req,
        key_portion[0],
        key_portion[1],
        request_index(key_tokens // F_TOK, counts, 1),
    )
    returned = lax.all_to_all(
        lax.all_to_all(normalize(folded), "seq", split_axis=0, concat_axis=1, tiled=True),
        "tp",
        split_axis=1,
        concat_axis=0,
        tiled=True,
    )
    flattened = returned.reshape(returned.shape[0], returned.shape[1] * returned.shape[2])
    summed = lax.psum_scatter(
        jnp.dot(flattened, out_weight, preferred_element_type=jnp.float32).astype(jnp.bfloat16),
        "tp",
        scatter_dimension=0,
        tiled=True,
    ).astype(jnp.float32)
    mixed_stream = stream[0].astype(jnp.float32) + summed
    average = jnp.mean(mixed_stream, axis=1, keepdims=True)
    centred = mixed_stream - average
    variance = jnp.mean(centred * centred, axis=1, keepdims=True)
    normed = centred / jnp.sqrt(variance + EPSILON)
    modulated = (normed * (1.0 + mod_scale[0]) + mod_shift[0]).astype(jnp.bfloat16)
    velocity = jnp.dot(modulated, final_weight, preferred_element_type=jnp.float32)
    updated = latent[0] + step_size[0] * velocity
    frame_local = token_rows // F_TOK
    own_video = updated.reshape(frame_local, PROWS, PCOLS, 2, 2, LATC).transpose(0, 1, 3, 2, 4, 5)
    own_video = own_video.reshape(frame_local, LROWS, LCOLS, LATC).astype(jnp.bfloat16)
    matched_pairs = lax.all_gather(own_video, "tp", axis=0, tiled=True)
    slab_grouped = lax.all_to_all(matched_pairs, "seq", split_axis=1, concat_axis=0, tiled=True)
    frame_count_total = slab_grouped.shape[0]
    rows_per_slab = slab_grouped.shape[1]
    with_halo_rows = padded_2(slab_grouped, (("seq", 1),), 1)
    padded = jnp.pad(with_halo_rows, ((2, 0), (0, 0), (1, 1), (0, 0)))
    frame_ids = jnp.arange(frame_count_total, dtype=jnp.int32)
    owner_req = request_index(frame_ids, counts, 1)
    starts = jnp.cumsum(counts) - counts
    selector = owner_req[:, None] == jnp.arange(counts.shape[0], dtype=jnp.int32)[None, :]
    first_frame = jnp.sum(jnp.where(selector, starts[None, :], 0), axis=1)
    alive_frame = jnp.sum(jnp.where(selector, done_flags[None, :], 0), axis=1)
    columns_list = []
    for time_tap in range(3):
        inside = frame_ids - 2 + time_tap >= first_frame
        for row_tap in range(3):
            for col_tap in range(3):
                window = padded[
                    time_tap : time_tap + frame_count_total,
                    row_tap : row_tap + rows_per_slab,
                    col_tap : col_tap + LCOLS,
                ]
                columns_list.append(
                    jnp.where(inside[:, None, None, None], window, jnp.zeros_like(window))
                )
    stacked = jnp.concatenate(columns_list, axis=3).reshape(-1, 27 * LATC)
    whole_kernel, whole_bias = (
        lax.all_gather(
            conv_weight.astype(jnp.float32).astype(jnp.bfloat16), "tp", axis=4, tiled=True
        ).astype(jnp.float32),
        lax.all_gather(conv_bias.astype(jnp.bfloat16), "tp", axis=0, tiled=True).astype(
            conv_bias.dtype
        ),
    )
    kernel = whole_kernel.astype(jnp.bfloat16).reshape(27 * LATC, whole_kernel.shape[4])
    hidden = jax.nn.silu(
        jnp.dot(stacked, kernel, preferred_element_type=jnp.float32) + whole_bias
    ).astype(jnp.bfloat16)
    own_columns = lax.all_to_all(up_weight, "tp", split_axis=1, concat_axis=0, tiled=True)
    shared = jnp.dot(hidden, own_columns, preferred_element_type=jnp.float32).reshape(
        frame_count_total, rows_per_slab, LCOLS, own_columns.shape[1]
    )
    decoded = ((shared + up_bias) * alive_frame.astype(jnp.float32)[:, None, None, None]).astype(
        jnp.bfloat16
    )
    return (updated[None], decoded[None])


NN = (((1,), (0,)), ((), ()))
NT = (((1,), (1,)), ((), ()))


def request_of(frame, ends):
    owner = (frame >= ends[0]).astype(jnp.int32)
    for end in ends[1:]:
        owner = owner + (frame >= end).astype(jnp.int32)
    return owner


def frame_ends(counts_ref, requests):
    ends = [counts_ref[0, 0]]
    for i in range(1, requests):
        ends.append(ends[-1] + counts_ref[0, i])
    return ends


def slab_start(seq, rows):
    return jnp.clip(seq * rows - 1, 0, PROWS - rows - 2)


def expand_weight(kernel_ref, expanded_ref, patch):
    for i in range(2):
        for j in range(2):
            for a in range(3):
                for dr in range(2):
                    for dc in range(2):
                        for i2 in range(2):
                            for j2 in range(2):
                                b = i - 1 + 2 * dr + i2
                                e = j - 1 + 2 * dc + j2
                                if 0 <= b < 3 and 0 <= e < 3:
                                    to = ((a * 2 + dr) * 2 + dc) * patch + (i2 * 2 + j2) * LATC
                                    come = ((a * 3 + b) * 3 + e) * LATC
                                    expanded_ref[i * 2 + j, to : to + LATC] = kernel_ref[come : come + LATC]


def attend_kernel(
    n,
    requests,
    qkv_ref,
    stream_ref,
    ow_ref,
    scale_hbm,
    shift_hbm,
    fw_hbm,
    latent_hbm,
    step_hbm,
    counts_hbm,
    finished_hbm,
    cw_ref,
    cb_ref,
    uw_ref,
    ub_hbm,
    new_latent_ref,
    decoded_ref,
    video_ref,
    expanded_ref,
    cb2_ref,
    uw2_ref,
    ub_ref,
    shifted,
    columns,
    spread,
    cw2_ref,
    scale_ref,
    shift_ref,
    fw_ref,
    latent_ref,
    step_ref,
    counts_ref,
    finished_ref,
    units,
    give,
    outgoing,
    incoming,
    w_buf,
    stream_buf,
    bias_buf,
    att_buf,
    acc_buf,
    part_buf,
    got_buf,
    mixed_buf,
    own_video,
    local_sems,
    swap_send,
    swap_recv,
    unit_send,
    unit_recv,
    part_send,
    part_recv,
    wt_send,
    wt_recv,
    vid_send,
    vid_recv,
):
    s = lax.axis_index("seq")
    t = lax.axis_index("tp")
    o = 1 - t
    me = s * 2 + t
    devices = 2 * n
    groups = units.shape[0]
    lanes = units.shape[4]
    out_half = uw_ref.shape[1] // 2
    ccols = cw_ref.shape[1]
    has_left = s > 0
    has_right = s < n - 1

    def at(seq, tp):
        return {"seq": seq, "tp": tp}

    def remote(src, dst, send, recv, target):
        return pltpu.make_async_remote_copy(
            src_ref=src,
            dst_ref=dst,
            send_sem=send,
            recv_sem=recv,
            device_id=target,
            device_id_type=pl.DeviceIdType.MESH,
        )

    def peer_of(k):
        peer = lax.rem(me + k, devices)
        return at(peer // 2, lax.rem(peer, 2))

    def cols(which, width):
        return pl.ds(pl.multiple_of(which * width, width), width)

    get_counts = pltpu.make_async_copy(counts_hbm, counts_ref, local_sems.at[0])
    get_finished = pltpu.make_async_copy(finished_hbm, finished_ref, local_sems.at[1])
    get_w = pltpu.make_async_copy(ow_ref, w_buf, local_sems.at[2])
    get_stream = pltpu.make_async_copy(stream_ref, stream_buf, local_sems.at[3])
    theirs = [
        pltpu.make_async_copy(
            qkv_ref.at[:, :, cols(o * groups + c, lanes)], give.at[c], local_sems.at[13 + c]
        )
        for c in range(groups)
    ]
    own = [
        pltpu.make_async_copy(
            qkv_ref.at[:, :, cols(t * groups + c, lanes)], units.at[c, t], local_sems.at[13 + groups + c]
        )
        for c in range(groups)
    ]
    for c in range(groups):
        theirs[c].start()
    for c in range(groups):
        own[c].start()
    get_counts.start()
    get_finished.start()

    barrier = pltpu.get_barrier_semaphore()
    for k in range(1, devices):
        pl.semaphore_signal(
            barrier, inc=1, device_id=peer_of(k), device_id_type=pl.DeviceIdType.MESH
        )
    pl.semaphore_wait(barrier, devices - 1)

    swaps = [
        remote(give.at[c], units.at[c, t], swap_send.at[c], swap_recv.at[c], at(s, o))
        for c in range(groups)
    ]
    for c in range(groups):
        theirs[c].wait()
        swaps[c].start()

    get_counts.wait()
    get_finished.wait()
    ends = frame_ends(counts_ref, requests)

    def request(frame):
        return jnp.where(frame < 0, -1, request_of(frame, ends))

    req = {k: request(s * 2 + k) for k in range(-2, 4)}
    left_tied = req[-1] == req[0]
    right_tied = req[1] == req[2]
    left_two = req[-2] == req[-1]
    own_two = req[0] == req[1]
    right_two = req[2] == req[3]
    pair_left = jnp.logical_and(left_tied, jnp.logical_and(left_two, own_two))
    pair_right = jnp.logical_and(right_tied, jnp.logical_and(own_two, right_two))
    paired = jnp.logical_or(pair_left, pair_right)
    away_left = jnp.logical_and(left_tied, jnp.logical_and(left_two, jnp.logical_not(own_two)))
    away_right = jnp.logical_and(right_tied, jnp.logical_not(own_two))
    pairs = (pair_left, pair_right)

    def pair_unit(u):
        place = u % 4
        return units[u // 4, place % 2, 1 + place // 2]

    def guest_unit(side, u):
        return units[u // 3, side, u % 3]

    guest_units = 3 * groups
    sends = [[], []]
    for u in range(4 * groups):
        for side, step in ((0, -1), (1, 1)):
            sends[side].append(
                remote(
                    outgoing.at[side, u],
                    incoming.at[1 - side, u],
                    unit_send.at[side, u],
                    unit_recv.at[1 - side, u],
                    at(s + step, t),
                )
            )

    def start(first, count):
        @pl.when(has_right)
        def _():
            for u in range(first, first + count):
                sends[1][u].start()

        @pl.when(has_left)
        def _():
            for u in range(first, first + count):
                sends[0][u].start()

    def arrived(first, count):
        @pl.when(has_left)
        def _():
            for u in range(first, first + count):
                remote(
                    incoming.at[0, u], incoming.at[0, u], unit_send.at[0, u], unit_recv.at[0, u], at(s, o)
                ).wait_recv()

        @pl.when(has_right)
        def _():
            for u in range(first, first + count):
                remote(
                    incoming.at[1, u], incoming.at[1, u], unit_send.at[1, u], unit_recv.at[1, u], at(s, o)
                ).wait_recv()

    for c in range(groups):
        own[c].wait()
        swaps[c].wait_recv()
        for u in range(3 * c, 3 * c + 3):
            for side in range(2):
                outgoing[side, u] = lax.select(pairs[side], pair_unit(u), guest_unit(side, u))
        start(3 * c, 3)

    give_cw = remote(cw_ref, cw2_ref.at[:, ccols:], wt_send.at[0], wt_recv.at[0], at(s, o))
    give_cb = remote(cb_ref, cb2_ref.at[:, ccols:], wt_send.at[1], wt_recv.at[1], at(s, o))
    give_uw = remote(
        uw_ref.at[:, cols(o, out_half)],
        uw2_ref.at[pl.ds(uw_ref.shape[0], uw_ref.shape[0])],
        wt_send.at[2],
        wt_recv.at[2],
        at(s, o),
    )
    give_cw.start()
    give_cb.start()
    give_uw.start()
    loads = [
        pltpu.make_async_copy(source, target, local_sems.at[4 + i])
        for i, (source, target) in enumerate(
            (
                (cw_ref, cw2_ref.at[:, :ccols]),
                (cb_ref, cb2_ref.at[:, :ccols]),
                (uw_ref.at[:, cols(t, out_half)], uw2_ref.at[: uw_ref.shape[0]]),
                (scale_hbm, scale_ref),
                (shift_hbm, shift_ref),
                (fw_hbm, fw_ref),
                (latent_hbm, latent_ref),
                (step_hbm, step_ref),
                (ub_hbm, ub_ref),
            )
        )
    ]
    for load in loads:
        load.start()
    get_stream.start()
    get_w.start()

    @pl.when(jnp.logical_not(has_left))
    def _():
        incoming[0] = jnp.zeros(incoming.shape[1:], incoming.dtype)

    @pl.when(jnp.logical_not(has_right))
    def _():
        incoming[1] = jnp.zeros(incoming.shape[1:], incoming.dtype)

    def fill_bias(which, rows, keys, open_ends):
        for i, row in enumerate(rows):
            for j, key in enumerate(keys):
                allowed = req[row] == req[key]
                if open_ends and j in (0, 3):
                    allowed = jnp.logical_or(paired, allowed)
                bias = jnp.where(allowed, 0.0, NEG_FILL).astype(jnp.float32)
                bias_buf[which, pl.ds(i * F_TOK, F_TOK), pl.ds(j * F_TOK, F_TOK)] = jnp.full(
                    (F_TOK, F_TOK), bias, jnp.float32
                )

    fill_bias(0, (0, 1), (-1, 0, 1, 2), True)
    fill_bias(1, (-1, 2), (-1, 0, 1, 2), False)
    score_scale = 1.0 / math.sqrt(HD)

    def weigh(queries, keys, which):
        scores = lax.dot_general(queries, keys, NT, preferred_element_type=jnp.float32)
        scores = scores * score_scale + bias_buf[which]
        weights = jnp.exp(scores - jnp.max(scores, axis=1, keepdims=True))
        return weights.astype(jnp.bfloat16), jnp.sum(weights, axis=1, keepdims=True)

    def gather(weights, total, values):
        product = lax.dot_general(weights, values, NN, preferred_element_type=jnp.float32)
        return (product / total).astype(jnp.bfloat16)

    def head(h):
        return pl.ds(h * HD, HD)

    heads = range(lanes // HD)

    def attend_guests(c):
        for h in heads:
            span = head(h)

            def joined(which):
                return jnp.concatenate(
                    [
                        incoming[0, 3 * c + which, :, span],
                        units[c, 0, which, :, span],
                        units[c, 1, which, :, span],
                        incoming[1, 3 * c + which, :, span],
                    ],
                    axis=0,
                )

            queries = jnp.concatenate([incoming[0, 3 * c, :, span], incoming[1, 3 * c, :, span]], axis=0)
            weights, total = weigh(queries, joined(1), 1)
            result = gather(weights, total, joined(2))
            u = guest_units + c
            place = u % 4
            pair = units[u // 4, place % 2, 1 + place // 2, :, span]
            for side in range(2):
                outgoing[side, u, :, span] = lax.select(
                    pairs[side], pair, result[side * F_TOK : (side + 1) * F_TOK]
                )
        start(guest_units + c, 1)

    def far(c, which, end, span):
        u = 4 * c + 2 * (which - 1) + end
        other = incoming[end, 3 * c + which, :, span]
        other = lax.select(pair_right, incoming[1, u, :, span], other)
        return lax.select(pair_left, incoming[0, u, :, span], other)

    def joined_own(c, which, span):
        return jnp.concatenate(
            [
                far(c, which, 0, span),
                units[c, 0, which, :, span],
                units[c, 1, which, :, span],
                far(c, which, 1, span),
            ],
            axis=0,
        )

    def weigh_own(c):
        found = []
        for h in heads:
            queries = jnp.concatenate([units[c, 0, 0, :, head(h)], units[c, 1, 0, :, head(h)]], axis=0)
            found.append(weigh(queries, joined_own(c, 1, head(h)), 0))
        return found

    def gather_own(c, found):
        for h in heads:
            weights, total = found[h]
            att_buf[c, :, head(h)] = gather(weights, total, joined_own(c, 2, head(h)))

    def attended(c):
        u = guest_units + c
        return jnp.concatenate(
            [
                lax.select(away_left, incoming[0, u], att_buf[c, :F_TOK]),
                lax.select(away_right, incoming[1, u], att_buf[c, F_TOK:]),
            ],
            axis=0,
        )

    chunks, _, chunk = part_buf.shape

    def project(first, count):
        ready = jnp.concatenate([attended(c) for c in range(first, first + count)], axis=1)
        rows = pl.ds(first * lanes, count * lanes)
        for j in range(chunks):
            span = pl.ds(j * chunk, chunk)
            result = lax.dot_general(ready, w_buf[rows, span], NN, preferred_element_type=jnp.float32)
            acc_buf[:, span] = result if first == 0 else acc_buf[:, span] + result

    loads[0].wait()
    give_cw.wait()
    expanded_ref[...] = jnp.zeros_like(expanded_ref)
    expand_weight(cw2_ref, expanded_ref, new_latent_ref.shape[0])

    arrived(0, 3)
    attend_guests(0)
    arrived(3, 1)
    gather_own(0, weigh_own(0))
    arrived(4, 2)
    attend_guests(1)
    arrived(6, 2)
    gather_own(1, weigh_own(1))
    arrived(8, 1)
    attend_guests(2)
    arrived(9, 3)
    attend_guests(3)
    gather_own(2, weigh_own(2))
    get_w.wait()
    get_stream.wait()
    for load in loads[1:]:
        load.wait()
    arrived(12, 2)
    project(0, 2)
    found = weigh_own(3)
    arrived(14, 1)
    project(2, 1)
    arrived(15, 1)
    gather_own(3, found)

    ready = attended(3)
    parts = []
    for c in range(chunks):
        span = pl.ds(c * chunk, chunk)
        result = acc_buf[:, span] + lax.dot_general(
            ready, w_buf[pl.ds(3 * lanes, lanes), span], NN, preferred_element_type=jnp.float32
        )
        first_rows, second_rows = result[:F_TOK], result[F_TOK:]
        part_buf[c] = lax.select(t == 0, second_rows, first_rows).astype(jnp.bfloat16)
        copy = remote(part_buf.at[c], got_buf.at[c], part_send.at[c], part_recv.at[c], at(s, o))
        copy.start()
        parts.append(copy)
        mixed_buf[:, span] = lax.select(t == 0, first_rows, second_rows) + stream_buf[:, span].astype(
            jnp.float32
        )
    row_sum = jnp.zeros((F_TOK, 1), jnp.float32)
    for c in range(chunks):
        span = pl.ds(c * chunk, chunk)
        parts[c].wait_recv()
        mixed = mixed_buf[:, span] + got_buf[c].astype(jnp.float32)
        mixed_buf[:, span] = mixed
        row_sum = row_sum + jnp.sum(mixed, axis=1, keepdims=True)
    width = mixed_buf.shape[1]
    average = row_sum / width
    row_square = jnp.zeros((F_TOK, 1), jnp.float32)
    for c in range(chunks):
        centred = mixed_buf[:, c * chunk : (c + 1) * chunk] - average
        row_square = row_square + jnp.sum(centred * centred, axis=1, keepdims=True)
    inverse = 1.0 / jnp.sqrt(row_square / width + EPSILON)
    velocity = jnp.zeros((fw_ref.shape[0], F_TOK), jnp.float32)
    for c in range(chunks):
        span = pl.ds(c * chunk, chunk)
        normed = (mixed_buf[:, span] - average) * inverse
        modulated = (normed * (1.0 + scale_ref[:, span]) + shift_ref[:, span]).astype(jnp.bfloat16)
        velocity = velocity + lax.dot_general(
            fw_ref[:, span], modulated, NT, preferred_element_type=jnp.float32
        )
    updated = latent_ref[...] + step_ref[0, 0] * velocity
    new_latent_ref[...] = updated
    own_video[...] = updated.T.astype(jnp.bfloat16)
    kept = video_ref.shape[1]

    def needed(seq):
        first = slab_start(seq, kept // PCOLS - 2) * PCOLS
        return pl.ds(pl.multiple_of(first, PCOLS), kept)

    videos = []
    for k in range(1, devices):
        target = peer_of(k)
        copy = remote(
            own_video.at[needed(target["seq"])],
            video_ref.at[me],
            vid_send.at[k - 1],
            vid_recv.at[k - 1],
            target,
        )
        copy.start()
        videos.append(copy)
    video_ref[me] = own_video[needed(s), :]

    for copy in swaps:
        copy.wait_send()

    @pl.when(has_right)
    def _():
        for copy in sends[1]:
            copy.wait_send()

    @pl.when(has_left)
    def _():
        for copy in sends[0]:
            copy.wait_send()

    for copy in parts:
        copy.wait_send()
    give_cb.wait()
    give_uw.wait()
    for copy in videos:
        copy.wait()
    decode_frames(
        kept // PCOLS - 2,
        requests,
        video_ref,
        expanded_ref,
        cb2_ref,
        uw2_ref,
        ub_ref,
        counts_ref,
        finished_ref,
        decoded_ref,
        shifted,
        columns,
        spread,
    )


def decode_frames(
    rows,
    requests,
    video_ref,
    expanded,
    cb_ref,
    uw_ref,
    ub_ref,
    counts_ref,
    finished_ref,
    out_ref,
    shifted,
    columns,
    spread,
):
    s = lax.axis_index("seq")
    frames = video_ref.shape[0]
    group = rows + 2
    span = group * PCOLS
    patch = video_ref.shape[2]
    ends = frame_ends(counts_ref, requests)
    owners = [request_of(jnp.int32(f), ends) for f in range(frames)]

    pieces = []
    for f in range(frames):
        for r in range(group):
            row = s * rows + r - 1
            inside = jnp.logical_and(row >= 0, row < PROWS)
            clamped = jnp.clip(row, 0, PROWS - 1) - slab_start(s, rows)
            piece = video_ref[f, pl.ds(pl.multiple_of(clamped * PCOLS, PCOLS), PCOLS), :]
            pieces.append(jnp.where(inside, piece.astype(jnp.float32), 0.0))
    middle = jnp.concatenate(pieces, axis=0)
    total = frames * span
    column = lax.rem(lax.broadcasted_iota(jnp.int32, (total, patch), 0), PCOLS)
    before = jnp.where(column == 0, 0.0, pltpu.roll(middle, 1, 0))
    after = jnp.where(column == PCOLS - 1, 0.0, pltpu.roll(middle, total - 1, 0))
    shifted[0] = jnp.concatenate([before, middle], axis=1).astype(jnp.bfloat16)
    shifted[1] = jnp.concatenate([middle, after], axis=1).astype(jnp.bfloat16)

    block = rows * PCOLS
    lanes = 2 * patch
    for f in range(frames):
        for a in range(3):
            g = f - 2 + a
            for i in range(2):
                for dr in range(2):
                    for j in range(2):
                        place = pl.ds((a * 2 + dr) * lanes, lanes)
                        if g < 0:
                            value = jnp.zeros((block, lanes), jnp.bfloat16)
                        else:
                            first = g * span + (i + dr) * PCOLS
                            value = shifted[j, first : first + block]
                            if g != f:
                                keep = (owners[g] == owners[f]).astype(jnp.float32)
                                value = value * jnp.full((1, lanes), keep, jnp.float32).astype(
                                    jnp.bfloat16
                                )
                        columns[i * 2 + j, f * block : (f + 1) * block, place] = value

    alive = []
    for f in range(frames):
        flag = jnp.float32(0)
        for r in range(requests):
            flag = flag + jnp.where(owners[f] == r, finished_ref[0, r], 0).astype(jnp.float32)
        alive.append(flag)
    out_cols = uw_ref.shape[1]
    for i in range(2):
        for j in range(2):
            hidden = lax.dot_general(
                columns[i * 2 + j], expanded[i * 2 + j], NN, preferred_element_type=jnp.float32
            )
            hidden = jax.nn.silu(hidden + cb_ref[...]).astype(jnp.bfloat16)
            shared = lax.dot_general(hidden, uw_ref[...], NN, preferred_element_type=jnp.float32)
            shared = shared + ub_ref[...]
            for f in range(frames):
                for r in range(rows):
                    first = f * block + r * PCOLS
                    value = shared[first : first + PCOLS] * alive[f]
                    for c in range(out_cols // 128):
                        spread[c, f, 2 * r + i, pl.ds(j, PCOLS, stride=2), :] = value[
                            :, c * 128 : (c + 1) * 128
                        ]
    for c in range(out_cols // 128):
        out_ref[:, :, :, c * 128 : (c + 1) * 128] = spread[c].astype(jnp.bfloat16)


def on_device_fast(
    qkv,
    stream,
    out_weight,
    mod_scale,
    mod_shift,
    final_weight,
    latent,
    step_size,
    frame_counts,
    finished,
    conv_weight,
    conv_bias,
    up_weight,
    up_bias,
):
    n = lax.axis_size("seq")
    frames = 2 * n
    requests = frame_counts.shape[1]
    width = stream.shape[2]
    patch = latent.shape[2]
    half = out_weight.shape[0]
    ccols = conv_weight.shape[4]
    taps = conv_weight.shape[0] * conv_weight.shape[1] * conv_weight.shape[2] * LATC
    up_rows, up_all = up_weight.shape
    out_half = up_all // 2
    groups = 4
    lanes = half // groups
    rows = PROWS // n
    chunks = 6
    chunk = width // chunks
    vmem = pl.BlockSpec(memory_space=pltpu.VMEM)
    anyspace = pl.BlockSpec(memory_space=pltpu.HBM)
    bf16, f32 = jnp.bfloat16, jnp.float32
    dma = pltpu.SemaphoreType.DMA
    new_latent, decoded = pl.pallas_call(
        lambda *refs: attend_kernel(n, requests, *refs),
        name="attend",
        out_shape=(
            jax.ShapeDtypeStruct((patch, F_TOK), f32),
            jax.ShapeDtypeStruct((frames, 2 * rows, LCOLS, out_half), bf16),
        ),
        in_specs=[
            anyspace,
            anyspace,
            anyspace,
            anyspace,
            anyspace,
            anyspace,
            anyspace,
            anyspace,
            anyspace,
            anyspace,
            anyspace,
            anyspace,
            anyspace,
            anyspace,
        ],
        out_specs=(vmem,) * 2,
        scratch_shapes=[
            pltpu.VMEM((frames, (rows + 2) * PCOLS, patch), bf16),
            pltpu.VMEM((4, 12 * patch, 2 * ccols), bf16),
            pltpu.VMEM((1, 2 * ccols), f32),
            pltpu.VMEM((2 * up_rows, out_half), bf16),
            pltpu.VMEM((1, out_half), f32),
            pltpu.VMEM((2, frames * (rows + 2) * PCOLS, 2 * patch), bf16),
            pltpu.VMEM((4, frames * rows * PCOLS, 12 * patch), bf16),
            pltpu.VMEM((out_half // 128, frames, 2 * rows, LCOLS, 128), f32),
            pltpu.VMEM((taps, 2 * ccols), bf16),
            pltpu.VMEM((1, width), f32),
            pltpu.VMEM((1, width), f32),
            pltpu.VMEM((patch, width), bf16),
            pltpu.VMEM((patch, F_TOK), f32),
            pltpu.SMEM((1, 1), f32),
            pltpu.SMEM((1, requests), jnp.int32),
            pltpu.SMEM((1, requests), jnp.int32),
            pltpu.VMEM((groups, 2, 3, F_TOK, lanes), bf16),
            pltpu.VMEM((groups, 3, F_TOK, lanes), bf16),
            pltpu.VMEM((2, 4 * groups, F_TOK, lanes), bf16),
            pltpu.VMEM((2, 4 * groups, F_TOK, lanes), bf16),
            pltpu.VMEM((half, width), bf16),
            pltpu.VMEM((F_TOK, width), bf16),
            pltpu.VMEM((2, 2 * F_TOK, 4 * F_TOK), f32),
            pltpu.VMEM((groups, 2 * F_TOK, lanes), bf16),
            pltpu.VMEM((2 * F_TOK, width), f32),
            pltpu.VMEM((chunks, F_TOK, chunk), bf16),
            pltpu.VMEM((chunks, F_TOK, chunk), bf16),
            pltpu.VMEM((F_TOK, width), f32),
            pltpu.VMEM((F_TOK, patch), bf16),
            dma((13 + 2 * groups,)),
            dma((groups,)),
            dma((groups,)),
            dma((2, 4 * groups)),
            dma((2, 4 * groups)),
            dma((chunks,)),
            dma((chunks,)),
            dma((3,)),
            dma((3,)),
            dma((2 * n - 1,)),
            dma((2 * n - 1,)),
        ],
        compiler_params=pltpu.CompilerParams(
            collective_id=0, has_side_effects=True, vmem_limit_bytes=41943040
        ),
    )(
        *(
            value if value.size == 1 else pltpu.with_memory_space_constraint(value, pltpu.HBM)
            for value in (
                qkv[0].transpose(1, 0, 2),
                stream[0],
                out_weight,
                mod_scale,
                mod_shift,
                final_weight.T,
                latent[0].T,
                step_size[None],
                frame_counts,
                finished,
                conv_weight.reshape(taps, ccols),
                conv_bias[None],
                up_weight,
                up_bias[None],
            )
        )
    )
    return (new_latent.T[None], decoded[None])


def solution(mesh):
    fast = mesh.shape["seq"] == 4 and mesh.shape["tp"] == 2
    in_specs = (
        P(("groups", "section"), ("seq", "tp"), None, None),
        P(("groups", "section"), ("seq", "tp"), None),
        P("tp", None),
        P(("groups", "section"), None),
        P(("groups", "section"), None),
        P(),
        P(("groups", "section"), ("seq", "tp"), None),
        P(("groups", "section")),
        P(("groups", "section"), None),
        P(("groups", "section"), None),
        P(None, None, None, None, "tp"),
        P("tp"),
        P("tp", None),
        P("tp"),
    )
    out_specs = (
        P(("groups", "section"), ("seq", "tp"), None),
        P(("groups", "section"), None, "seq", None, "tp"),
    )
    return jax.shard_map(
        on_device_fast if fast else on_device, mesh=mesh, in_specs=in_specs, out_specs=out_specs, check_vma=False
    )
```
